32 devices in a mesh: row: 4 (over y, core), col: 8 (over z, x).
Axes of the slice: x: 2, y: 2, z: 4, core: 2. Of those that a mesh axis runs over, the one named last changes fastest.
Arguments:
- l_saved: bfloat16 [16, 4, 256, 8, 256], P(None, 'row', None, 'col'), as said below
- l_grad: bfloat16 [16, 4, 256, 8, 256], P(None, 'row', None, 'col'), as said below
Outputs:
- grad_out: float32 [16, 4, 256, 8, 256], P(None, 'row', None, 'col')
Inputs may be any that keep to these rules, and one draw needn't show every extreme that they name: Read as one matrix of 16384 rows, l_saved is lower triangular with its diagonal between 1 and 2. Read as one matrix, l_grad is zero above the diagonal.
All inputs are finite; a program needn't handle non-finite values.
Results may differ from the reference program's by a relative error of at most 0.0003.
Values may be sent and summed in bfloat16 or wider, within the bound.
No kernel may reach another device: no remote copies, remote signals or barrier semaphores. Data moves between devices by JAX's collectives and lax.ppermute only.
A program may use at most 64 MiB of HBM per device.

```python
import jax
import jax.numpy as jnp
from jax import lax

TILE = 256
N = 16384
TR = 16
N_ROW = 4
N_COL = 8


def global_index(shape):
    tile_row = lax.broadcasted_iota(jnp.int32, shape, 0) * N_ROW + lax.broadcasted_iota(jnp.int32, shape, 1)
    rows = tile_row * TILE + lax.broadcasted_iota(jnp.int32, shape, 2)
    cols = lax.broadcasted_iota(jnp.int32, shape, 3) * TILE + lax.broadcasted_iota(jnp.int32, shape, 4)
    return (rows, cols)


def draw_l_saved(key, part):
    shape = (TR, N_ROW, TILE, N_COL, TILE)
    rows, cols = global_index(shape)
    first, second = jax.random.split(jax.random.fold_in(key, 11))
    base = jax.random.normal(first, shape, jnp.float32)
    same_tile = rows // TILE == cols // TILE
    spread = jnp.where(same_tile, 0.35 / TILE ** 0.5, (N * TILE) ** (-0.25))
    diagonal = jax.random.uniform(second, shape, jnp.float32, 1.0, 2.0)
    value = jnp.where(rows > cols, base * spread, jnp.where(rows == cols, diagonal, 0.0))
    return value.astype(jnp.bfloat16)


def draw_l_grad(key, part):
    shape = (TR, N_ROW, TILE, N_COL, TILE)
    rows, cols = global_index(shape)
    first = jax.random.fold_in(jax.random.fold_in(key, 23), 0)
    base = jax.random.normal(first, shape, jnp.float32)
    return jnp.where(rows >= cols, base, 0.0).astype(jnp.bfloat16)


def setup_inputs(seed: int = 0) -> dict:
    seeds = jax.random.split(jax.random.key(seed), 3)
    l_saved = draw_l_saved(jax.random.fold_in(seeds[2], 71), 0)
    l_grad = draw_l_grad(jax.random.fold_in(seeds[2], 71), 0)
    return dict(l_saved=l_saved, l_grad=l_grad)


HIGH = lax.Precision.HIGHEST

def right_solve(factor, rhs):
    return lax.linalg.triangular_solve(factor, rhs, left_side=False, lower=True)

def diag_gradient(factor, lower_part):
    eye = jnp.eye(factor.shape[0], dtype=jnp.float32)
    middle = jnp.dot(factor.T.astype(jnp.float32), lower_part.astype(jnp.float32), precision=HIGH, preferred_element_type=jnp.float32)
    middle = jnp.tril(middle) - 0.5 * middle * eye
    half = lax.linalg.triangular_solve(factor, middle, left_side=True, lower=True, transpose_a=True)
    full = right_solve(factor, half)
    return full + full.T

def stacked_inner(left, right):
    flat_left = left.reshape(-1, left.shape[-1])
    flat_right = right.reshape(-1, right.shape[-1]).astype(jnp.float32)
    return lax.dot_general(flat_left.astype(jnp.float32), flat_right.astype(jnp.float32), (((0,), (0,)), ((), ())), precision=HIGH, preferred_element_type=jnp.float32)

def reference(l_saved, l_grad):
    n_tiles = N // TILE
    n_cols = N_COL
    factor = l_saved.reshape(n_tiles, TILE, n_cols, TILE).transpose(0, 2, 1, 3)
    grad = l_grad.reshape(n_tiles, TILE, n_cols, TILE).transpose(0, 2, 1, 3).astype(jnp.float32)
    tile_ids = jnp.arange(n_tiles, dtype=jnp.int32)
    col_ids = jnp.arange(n_cols, dtype=jnp.int32)
    eye = jnp.eye(TILE, dtype=jnp.float32)
    for panel in (n_cols - 1, n_cols - 2):
        diag_factor = factor[panel, panel].astype(jnp.float32)
        inverse = right_solve(diag_factor, eye)
        below = (tile_ids > panel)[:, None, None]
        column = grad[:, panel]
        solved = jnp.dot(column.reshape(-1, TILE).astype(jnp.float32), inverse.astype(jnp.float32), precision=HIGH, preferred_element_type=jnp.float32).reshape(n_tiles, TILE, TILE)
        cbar = jnp.where(below, solved, jnp.float32(0.0))
        total = column[panel] - stacked_inner(cbar, factor[:, panel])
        sym = diag_gradient(diag_factor, jnp.tril(total))

        def one_column(kcol):
            row_factor = factor[panel, kcol].astype(jnp.float32)
            update = jnp.dot(cbar.reshape(-1, TILE).astype(jnp.float32), row_factor.astype(jnp.float32), precision=HIGH, preferred_element_type=jnp.float32)
            fresh = grad[:, kcol] - update.reshape(n_tiles, TILE, TILE)
            summed = stacked_inner(cbar, factor[:, kcol])
            own = grad[panel, kcol] - (summed + jnp.dot(sym.astype(jnp.float32), row_factor.astype(jnp.float32), precision=HIGH, preferred_element_type=jnp.float32))
            return fresh.at[panel].set(own)
        updated = lax.map(one_column, col_ids).transpose(1, 0, 2, 3)
        abar = jnp.tril(sym) - 0.5 * sym * eye
        panel_col = jnp.where(below, cbar, jnp.where((tile_ids == panel)[:, None, None], abar[None], jnp.float32(0.0)))
        grad = jnp.where((col_ids < panel)[None, :, None, None], updated, grad)
        grad = grad.at[:, panel].set(panel_col)
    return grad.transpose(0, 2, 1, 3).reshape(TR, N_ROW, TILE, N_COL, TILE)
```

```python
import functools

import jax
import jax.numpy as jnp
from jax import lax
from jax.experimental import pallas as pl
from jax.experimental.pallas import tpu as pltpu
from jax.sharding import PartitionSpec as P

F32 = jnp.float32
BF16 = jnp.bfloat16
VMEM = pl.BlockSpec(memory_space=pltpu.VMEM)
SMEM = pl.BlockSpec(memory_space=pltpu.SMEM)


def split(x):
    if x.dtype == BF16:
        return (x,)
    high = x.astype(BF16)
    return (high, (x - high.astype(F32)).astype(BF16))


def product(left, right, left_dim=1, right_dim=0):
    total = None
    for i, a in enumerate(split(left)):
        for j, b in enumerate(split(right)):
            if i + j < 2:
                term = lax.dot_general(
                    a, b, (((left_dim,), (right_dim,)), ((), ())), preferred_element_type=F32
                )
                total = term if total is None else total + term
    return total


def indices(tile):
    rows = lax.broadcasted_iota(jnp.int32, (tile, tile), 0)
    cols = lax.broadcasted_iota(jnp.int32, (tile, tile), 1)
    return rows, cols


def inverses(factors):
    tile = factors[0].shape[0]
    rows, cols = indices(tile)
    eye = rows == cols
    wide = [f.astype(F32) for f in factors]
    done = [jnp.where(eye, 1.0 / jnp.where(eye, f, 1.0), 0.0) for f in wide]
    size = 1
    while size < tile:
        pair = (rows // (2 * size) == cols // (2 * size)) & (rows // size != cols // size)
        parts = [jnp.where(pair, f, 0.0).astype(BF16) for f in wide]
        steps = [product(w, b) for w, b in zip(done, parts)]
        done = [w - product(s, w) for w, s in zip(done, steps)]
        size *= 2
    return done


def weights_kernel(place, l77, l76, l66, l7, l6, w7_ref, w6_ref, v_ref, high_ref, low_ref):
    tile = l77.shape[0]
    rows, cols = indices(tile)
    minus_eye = jnp.where(rows == cols, -1.0, 0.0)
    w7, w6 = inverses([l77[...], l66[...]])
    last, second = place[0] == 1, place[1] == 1
    row7 = jnp.where(last, minus_eye, jnp.where(second, 0.0, l7[...].astype(F32)))
    row6 = jnp.where(second, minus_eye, jnp.where(last, 0.0, l6[...].astype(F32)))
    x = product(w6, row6.astype(BF16))
    y = product(w7, row7 - product(l76[...], x))
    w7_ref[...] = w7
    w6_ref[...] = w6
    v_ref[...] = product(w7, l76[...])
    for k, value in enumerate((-y, -x)):
        high, low = split(value)
        high_ref[k * tile : (k + 1) * tile, :] = high
        low_ref[k * tile : (k + 1) * tile, :] = low


def weights(place, *tiles):
    tile = tiles[0].shape[0]
    square = jax.ShapeDtypeStruct((tile, tile), F32)
    tall = jax.ShapeDtypeStruct((2 * tile, tile), BF16)
    return pl.pallas_call(
        weights_kernel,
        out_shape=(square, square, square, tall, tall),
        in_specs=[SMEM] + [VMEM] * 5,
        out_specs=(VMEM,) * 5,
        cost_estimate=pl.CostEstimate(flops=120 * tile**3, bytes_accessed=8 * tile**2, transcendentals=0),
        name="weights",
    )(place, *tiles)


def gram_kernel(first, g7, g6, low, w7, w6, v, p_ref):
    tile = w7.shape[0]
    n = g7.shape[0]
    a7 = product(g7[...], low[first:, :], 0, 0)
    a6 = product(g6[...], low[first:, :], 0, 0)
    p_ref[:tile, :] = product(w7[...], a7, 0, 0)
    p_ref[tile:, :] = product(w6[...], a6 - product(v[...], a7, 0, 0), 0, 0)


def grams(first, g7, g6, low, w7, w6, v):
    tile = w7.shape[0]
    return pl.pallas_call(
        functools.partial(gram_kernel, first),
        out_shape=jax.ShapeDtypeStruct((2 * tile, tile), F32),
        in_specs=[VMEM] * 6,
        out_specs=VMEM,
        name="grams",
    )(g7, g6, low, w7, w6, v)


def symmetric(factor, inverse, lower):
    rows, cols = indices(factor.shape[0])
    middle = product(factor, lower, 0, 0)
    phi = jnp.where(rows > cols, middle, jnp.where(rows == cols, 0.5 * middle, 0.0))
    full = product(product(inverse, phi, 0, 0), inverse)
    return full + full.T


def halved(sym):
    rows, cols = indices(sym.shape[0])
    return jnp.where(rows > cols, sym, jnp.where(rows == cols, 0.5 * sym, 0.0))


def tail_kernel(place, t77, t76, t66, l77, l76, l66, w7, w6, l7, l6, g, p, out_ref):
    tile = g.shape[0]
    rows, cols = indices(tile)
    lower = rows >= cols
    last, second, top, bottom = (place[k] == 1 for k in range(4))
    s7 = symmetric(l77[...], w7[...], jnp.where(lower, t77[...], 0.0))
    c67 = product(t76[...] - product(s7, l76[...]), w6[...])
    q6 = jnp.where(lower, t66[...] - product(c67, l76[...], 0, 0), 0.0)
    s6 = symmetric(l66[...], w6[...], q6)
    from7 = jnp.where(top, s7, c67.T)
    from6 = jnp.where(top, c67, s6)
    panel = top | bottom
    gradient = g[...].astype(F32)
    part = jnp.where(top, p[:tile, :], p[tile:, :])
    fresh = gradient - part - product(from7, l7[...]) - product(from6, l6[...])
    left = jnp.where(panel, fresh, gradient)
    at6 = jnp.where(top, c67, jnp.where(bottom, halved(s6), 0.0))
    at7 = jnp.where(top, halved(s7), 0.0)
    out_ref[...] = jnp.where(last, at7, jnp.where(second, at6, left))


def tail(place, *arrays):
    tile = arrays[0].shape[0]
    return pl.pallas_call(
        tail_kernel,
        out_shape=jax.ShapeDtypeStruct((tile, tile), F32),
        in_specs=[SMEM] + [VMEM] * len(arrays),
        out_specs=VMEM,
        name="tail",
    )(place, *arrays)


def out_kernel(first, place, g, g7, g6, high, low, out_ref):
    tile = high.shape[1]
    half = tile // 2
    inside = place[4] == 1

    def put(row, value):
        out_ref[pl.ds(2 * row, tile, stride=2), :] = value[:, :half]
        out_ref[pl.ds(2 * row + 1, tile, stride=2), :] = value[:, half:]

    for t in range(first):
        row = t * tile
        put(row, jnp.where(inside, g[row : row + tile, :].astype(F32), 0.0))

    def step(t, carry):
        row = pl.multiple_of(t * tile, tile)
        total = jnp.where(inside, g[pl.ds(first * tile + row, tile), :].astype(F32), 0.0)
        for k, part in enumerate((g7, g6)):
            block = part[pl.ds(row, tile), :]
            for weight in (high, low):
                total += jnp.dot(
                    block, weight[k * tile : (k + 1) * tile, :], preferred_element_type=F32
                )
        put(first * tile + row, total)
        return carry

    lax.fori_loop(0, g7.shape[0] // tile, step, 0)


def outputs(first, place, g, g7, g6, high, low):
    n, tile = g.shape
    return pl.pallas_call(
        functools.partial(out_kernel, first),
        out_shape=jax.ShapeDtypeStruct((2 * n, tile // 2), F32),
        in_specs=[SMEM] + [VMEM] * 5,
        out_specs=VMEM,
        name="outputs",
    )(place, g, g7, g6, high, low)


def place_kernel(row, tile_ref, whole_ref, out_ref, stage, sem):
    n, tile = tile_ref.shape
    half = tile // 2
    stage[pl.ds(0, n, stride=2), :] = tile_ref[:, :half]
    stage[pl.ds(1, n, stride=2), :] = tile_ref[:, half:]
    copy = pltpu.make_async_copy(stage, out_ref.at[pl.ds(2 * row, 2 * n), :], sem)
    copy.start()
    copy.wait()


def place_tile(row, tile_value, whole):
    n, tile = tile_value.shape
    anywhere = pl.BlockSpec(memory_space=pl.ANY)
    return pl.pallas_call(
        functools.partial(place_kernel, row),
        out_shape=jax.ShapeDtypeStruct(whole.shape, F32),
        in_specs=[VMEM, anywhere],
        out_specs=anywhere,
        scratch_shapes=[pltpu.VMEM((2 * n, tile // 2), F32), pltpu.SemaphoreType.DMA],
        input_output_aliases={1: 0},
        name="place_tile",
    )(tile_value, whole)


def per_device(l_saved, l_grad):
    rows_here, tile = l_saved.shape[0], l_saved.shape[2]
    n_row, n_col = lax.axis_size("row"), lax.axis_size("col")
    if n_col % n_row or n_col % 2 or n_row & (n_row - 1) or n_row < 2:
        raise ValueError("mesh shape")
    first = n_col // n_row
    seven, six = n_col - 1, n_col - 2
    top_row, bottom_row = n_row - 1, n_row - 2
    my_row, my_col = lax.axis_index("row"), lax.axis_index("col")
    hop = (seven - my_col) // 2
    odd = my_col % 2 == seven % 2
    low = l_saved.reshape(rows_here * tile, tile)
    grad = l_grad.reshape(rows_here * tile, tile)
    last, second = my_col == seven, my_col == six
    top, bottom = my_row == top_row, my_row == bottom_row
    place = jnp.stack([last, second, top, bottom, my_col < six]).astype(jnp.int32)

    def down(x):
        reach = 1
        while reach < n_col // 2:
            pairs = [
                (c, c - 2 * reach)
                for c in range(n_col)
                if (seven - c) // 2 < reach and c >= 2 * reach
            ]
            y = lax.ppermute(x, "col", pairs)
            x = jnp.where((hop >= reach) & (hop < 2 * reach), y, x)
            reach *= 2
        return x

    def swap(x):
        return lax.ppermute(x, "col", [(c, c ^ 1) for c in range(n_col)])

    def both(x):
        other = swap(x)
        return jnp.where(odd, x, other), jnp.where(odd, other, x)

    def row_sum(x):
        reach = 1
        while reach < n_row:
            x = x + lax.ppermute(x, "row", [(r, r ^ reach) for r in range(n_row)])
            reach *= 2
        return x

    edge = (first - 1) * tile
    row_tiles = lax.all_gather(low[edge : edge + tile], "row")
    l7, l6 = row_tiles[top_row], row_tiles[bottom_row]
    at7, at6 = both(down(jnp.concatenate([l7, l6], 0)))
    l77, l76, l66 = at7[:tile], at6[:tile], at6[tile:]
    w7, w6, v, high, lowp = weights(place, l77, l76, l66, l7, l6)

    g7, g6 = both(down(grad[first * tile :]))
    part = grams(first * tile, g7, g6, low, w7, w6, v)
    g_tile = grad[edge : edge + tile]
    mine = jnp.where(top & last, g_tile, jnp.zeros_like(g_tile)).astype(F32)
    upper = jnp.where(top & second, g_tile, jnp.zeros_like(g_tile)).astype(F32)
    under = jnp.where(bottom & second, g_tile, jnp.zeros_like(g_tile)).astype(F32)
    tiles = jnp.where(last, jnp.concatenate([mine, under], 0), jnp.concatenate([upper, under], 0)) - part
    total = row_sum(jnp.concatenate([tiles, part], 0))
    s7, s6 = both(down(total[: 2 * tile]))
    t77, t76, t66 = s7[:tile], s6[:tile], s6[tile:]
    tile_out = tail(place, t77, t76, t66, l77, l76, l66, w7, w6, l7, l6, g_tile, total[2 * tile :])
    whole = outputs(first, place, grad, g7, g6, high, lowp)
    whole = place_tile(edge, tile_out, whole)
    return whole.reshape(l_grad.shape)


def solution(mesh):
    spec = P(None, "row", None, "col", None)
    return jax.shard_map(
        per_device, mesh=mesh, in_specs=(spec, spec), out_specs=spec, check_vma=False
    )
```
